128 devices in a mesh: pb: 8 (over x, core), kv: 8 (over z_lo, y), ha: 2 (over z_hi).
Axes of the slice: x: 4, y: 4, z: 4 (z_hi: 2, z_lo: 2; z = z_hi * 2 + z_lo), core: 2. Of those that a mesh axis runs over, the one named last changes fastest.
Arguments:
- queries: bfloat16 [12288, 2048], P(('pb', 'kv', 'ha')), may hold values from -48 to 48
- keys: bfloat16 [12288, 2048], P(('pb', 'kv', 'ha')), may hold values from -6 to 6
- values: bfloat16 [12288, 2048], P(('pb', 'kv', 'ha')), may hold values from -6 to 6
- masked_at: int32 [3072], replicated, may hold values from 0 to 12287, as said below
- mask_query: bfloat16 [2048], replicated, may hold values from -6 to 6
- mask_key: bfloat16 [2048], replicated, may hold values from -6 to 6
- mask_value: bfloat16 [2048], replicated, may hold values from -6 to 6
Outputs:
- attended: bfloat16 [12288, 2048], P(('pb', 'kv', 'ha'))
The draws below stay inside these ranges and needn't reach their ends.
Inputs may be any that keep to these rules, and one draw needn't show every extreme that they name: `masked_at`: 3072 distinct positions in rising order.
All inputs are finite; a program needn't handle non-finite values.
Results may differ from the reference program's by a relative error of at most 0.006.
Values may be sent and summed in bfloat16 or wider, within the bound.
No kernel may reach another device: no remote copies, remote signals or barrier semaphores. Data moves between devices by JAX's collectives and lax.ppermute only.
A program may use at most 128 MiB of HBM per device.

```python
import math
import jax
import jax.numpy as jnp
from jax import lax

DH = 128
HEADS = 16
TOKENS = 12288
MASKED = 3072


def paired_fields(key):
    width = HEADS * DH
    key_field = jnp.clip(1.7 * jax.random.normal(jax.random.fold_in(key, 111), (TOKENS, width), jnp.float32), -6.0, 6.0)
    query_field = jnp.clip(1.7 * jax.random.normal(jax.random.fold_in(key, 112), (TOKENS, width), jnp.float32), -6.0, 6.0)
    return (query_field.astype(jnp.bfloat16), key_field.astype(jnp.bfloat16))


def draw_queries(key, part):
    return paired_fields(key)[0]


def draw_keys(key, part):
    return paired_fields(key)[1]


def draw_masked_at(key, part):
    chosen = jax.random.permutation(jax.random.fold_in(key, 121), TOKENS)[:MASKED]
    return jnp.sort(chosen).astype(jnp.int32)


def levels(key, dims, pieces, least, largest):
    factor_of, own = 1.0, jax.random.fold_in(key, 6)
    for dim, shards_of in pieces:
        steps = jnp.exp(jax.random.uniform(jax.random.fold_in(own, dim), (shards_of,), jnp.float32, least / len(pieces), largest / len(pieces)))
        factor_of = factor_of * jnp.repeat(steps, dims[dim] // shards_of).reshape([-1 if axis == dim else 1 for axis in range(len(dims))])
    return factor_of


def gaussian(own_key, shape, deviation, most, split=(), kind=jnp.bfloat16):
    drawn = jax.random.normal(own_key, shape, jnp.float32) * deviation
    if len(split) > 0:
        drawn = levels(own_key, shape, split, -0.22, 0.18) * drawn
    return jnp.clip(drawn, min=-most, max=most).astype(kind)


def setup_inputs(seed: int = 0) -> dict:
    arg_keys = jax.random.split(jax.random.key(seed), 8)
    queries = draw_queries(jax.random.fold_in(arg_keys[7], 71), 0)
    keys = draw_keys(jax.random.fold_in(arg_keys[7], 71), 0)
    values = gaussian(arg_keys[2], (TOKENS, HEADS * DH), 1.0, 6.0, ((0, 128),))
    masked_at = draw_masked_at(jax.random.fold_in(arg_keys[7], 71), 0)
    mask_query = gaussian(arg_keys[4], (HEADS * DH,), 1.7, 6.0)
    mask_key = gaussian(arg_keys[5], (HEADS * DH,), 1.7, 6.0)
    mask_value = gaussian(arg_keys[6], (HEADS * DH,), 1.0, 6.0)
    return {"queries": queries, "keys": keys, "values": values, "masked_at": masked_at, "mask_query": mask_query, "mask_key": mask_key, "mask_value": mask_value}


rope_theta = 500000.0

def rotated(vector, positions):
    halves = DH // 2
    exponent = jnp.arange(halves, dtype=jnp.float32) * (2.0 / DH)
    inverse = 1.0 / rope_theta ** exponent
    angles = positions.astype(jnp.float32)[:, None] * inverse[None, :]
    cosine = jnp.cos(angles)[:, None, :]
    sine_part = jnp.sin(angles)[:, None, :]
    per_head = vector.astype(jnp.float32).reshape(HEADS, DH)
    first_half = per_head[None, :, :halves]
    second = per_head[None, :, halves:]
    result = jnp.concatenate([first_half * cosine - second * sine_part, second * cosine + first_half * sine_part], axis=2)
    return result.reshape(positions.shape[0], HEADS * DH).astype(jnp.bfloat16)

def reference(queries, keys, values, masked_at, mask_query, mask_key, mask_value):
    positions = jnp.arange(TOKENS, dtype=jnp.int32)
    masked_flags = jnp.zeros((TOKENS,), jnp.int32).at[masked_at].set(1) > 0
    query_used = jnp.where(masked_flags[:, None], rotated(mask_query, positions), queries)
    key_used = jnp.where(masked_flags[:, None], rotated(mask_key, positions), keys)
    value_used = jnp.where(masked_flags[:, None], mask_value[None, :], values)
    block_rows = math.gcd(TOKENS, 1024)
    score_scale = 1.0 / math.sqrt(DH)

    def one_head(head_index):
        head_queries = lax.dynamic_slice_in_dim(query_used, head_index * DH, DH, 1)
        head_keys = lax.dynamic_slice_in_dim(key_used, head_index * DH, DH, 1)
        head_values = lax.dynamic_slice_in_dim(value_used, head_index * DH, DH, 1)

        def one_block(block_index):
            query_rows = lax.dynamic_slice_in_dim(head_queries, block_index * block_rows, block_rows, 0)
            scores = jnp.dot(query_rows, head_keys.T, preferred_element_type=jnp.float32) * score_scale
            maxima = lax.optimization_barrier(jnp.max(scores, axis=1))
            weights = jnp.exp(scores - maxima[:, None])
            totals = lax.optimization_barrier(jnp.sum(weights, axis=1))
            outputs = jnp.dot(weights.astype(jnp.bfloat16), head_values, preferred_element_type=jnp.float32)
            return (outputs / totals[:, None]).astype(jnp.bfloat16)
        blocks = lax.map(one_block, jnp.arange(TOKENS // block_rows, dtype=jnp.int32))
        return blocks.reshape(TOKENS, DH)
    stacked = lax.map(one_head, jnp.arange(HEADS, dtype=jnp.int32))
    return stacked.transpose(1, 0, 2).reshape(TOKENS, HEADS * DH)
```

```python
import functools
import math

import jax
import jax.numpy as jnp
from jax import lax
from jax.experimental import pallas as pl
from jax.experimental.pallas import tpu as pltpu
from jax.sharding import PartitionSpec as P

DH = 128
HEADS = 16
ROPE_THETA = 500000.0
VERY_NEGATIVE = -1e30
SAFE_SCORE = 100.0
SCORE_SCALE = math.log2(math.e) / math.sqrt(DH)
CONTRACT_LAST = (((1,), (1,)), ((), ()))
PLANE = ("kv", "ha")


def rotated(vector, positions):
    halves = DH // 2
    exponent = jnp.arange(halves, dtype=jnp.float32) * (2.0 / DH)
    inverse = 1.0 / ROPE_THETA**exponent
    angles = positions.astype(jnp.float32)[:, None] * inverse[None, :]
    cosine = jnp.cos(angles)[:, None, :]
    sine_part = jnp.sin(angles)[:, None, :]
    per_head = vector.astype(jnp.float32).reshape(HEADS, DH)
    first_half = per_head[None, :, :halves]
    second = per_head[None, :, halves:]
    result = jnp.concatenate(
        [first_half * cosine - second * sine_part, second * cosine + first_half * sine_part], axis=2
    )
    return result.reshape(positions.shape[0], HEADS * DH).astype(jnp.bfloat16)


def along_x(x, step):
    return lax.ppermute(x, "pb", [(i, (i + 2 * step) % 8) for i in range(8)])


def other_core(x):
    return lax.ppermute(x, "pb", [(i, i ^ 1) for i in range(8)])


def row_norm_max(rows):
    wide = rows.astype(jnp.float32)
    return jnp.max(jnp.sum(wide * wide, axis=1, keepdims=True))


def split_kernel(q_ref, out_ref, norm_ref):
    scaled = q_ref[...].astype(jnp.float32) * SCORE_SCALE
    high = scaled.astype(jnp.bfloat16)
    low = (scaled - high.astype(jnp.float32)).astype(jnp.bfloat16)
    out_ref[:, :DH] = high
    out_ref[:, DH:] = low
    norm_ref[0, 0] = row_norm_max(scaled)


def split_queries(q):
    rows = q.shape[0]
    return pl.pallas_call(
        split_kernel,
        in_specs=[pl.BlockSpec(memory_space=pltpu.VMEM)],
        out_specs=[pl.BlockSpec(memory_space=pltpu.VMEM), pl.BlockSpec(memory_space=pltpu.SMEM)],
        out_shape=[
            jax.ShapeDtypeStruct((rows, 2 * DH), jnp.bfloat16),
            jax.ShapeDtypeStruct((1, 1), jnp.float32),
        ],
        name="split_queries",
    )(q)


def attend_kernel(*refs, pieces, first, key_tile, query_tile):
    norm_ref, q_ref = refs[:2]
    key_refs = refs[2 : 2 + pieces]
    value_refs = refs[2 + pieces : 2 + 2 * pieces]
    rest = refs[2 + 2 * pieces :]
    if not first:
        flag_in, sum_in, total_in, max_in = rest[:4]
        rest = rest[4:]
    flag_out, sum_out, total_out, max_out, turned_ref, weight_ref, safe_ref = rest
    piece_rows = key_refs[0].shape[0]
    rows = q_ref.shape[0]

    @pl.when(pl.program_id(0) == 0)
    def _():
        largest = 0.0
        for piece in range(pieces):
            turned_ref[:, pl.ds(piece * piece_rows, piece_rows)] = value_refs[piece][...].T
            largest = jnp.maximum(largest, row_norm_max(key_refs[piece][...]))
        safe = (largest * norm_ref[0, 0] * 1.02 < SAFE_SCORE * SAFE_SCORE).astype(jnp.int32)
        if not first:
            safe = safe * flag_in[0, 0]
        safe_ref[0] = safe
        flag_out[0, 0] = safe

    def doubled(piece, start, size):
        tile = key_refs[piece][pl.ds(start, size), :]
        return jnp.concatenate([tile, tile], axis=1)

    @pl.when(safe_ref[0] == 1)
    def _():
        max_out[...] = jnp.zeros(max_out.shape, jnp.float32)
        for block in range(rows // query_tile):
            columns = pl.ds(block * query_tile, query_tile)
            queries = q_ref[columns, :]
            total = None if first else total_in[:, columns]
            for piece in range(pieces):
                for tile in range(piece_rows // key_tile):
                    scores = lax.dot_general(
                        doubled(piece, tile * key_tile, key_tile),
                        queries,
                        CONTRACT_LAST,
                        preferred_element_type=jnp.float32,
                    )
                    weights = jnp.exp2(scores)
                    part = weights.reshape(key_tile // 8, 8, query_tile).sum(axis=0)
                    total = part if total is None else total + part
                    weight_ref[block % 2, pl.ds(piece * piece_rows + tile * key_tile, key_tile), :] = (
                        weights.astype(jnp.bfloat16)
                    )
            summed = jnp.dot(turned_ref[...], weight_ref[block % 2], preferred_element_type=jnp.float32)
            if not first:
                summed = summed + sum_in[:, columns]
            sum_out[:, columns] = summed
            total_out[:, columns] = total

    @pl.when(safe_ref[0] == 0)
    def _():
        if first:
            sum_out[...] = jnp.zeros(sum_out.shape, jnp.float32)
            total_out[...] = jnp.zeros(total_out.shape, jnp.float32)
            max_out[...] = jnp.full(max_out.shape, VERY_NEGATIVE, jnp.float32)
        else:
            sum_out[...] = sum_in[...]
            total_out[...] = total_in[...]
            max_out[...] = max_in[...]
        small = 128
        for piece in range(pieces):

            def one_tile(index, carry):
                start = pl.multiple_of((index // (rows // small)) * small, small)
                columns = pl.ds(pl.multiple_of((index % (rows // small)) * small, small), small)
                scores = lax.dot_general(
                    doubled(piece, start, small),
                    q_ref[columns, :],
                    CONTRACT_LAST,
                    preferred_element_type=jnp.float32,
                )
                old_max = max_out[:1, columns]
                new_max = jnp.maximum(old_max, jnp.max(scores, axis=0, keepdims=True))
                factor = jnp.exp2(old_max - new_max)
                weights = jnp.exp2(scores - new_max)
                total_out[:, columns] = total_out[:, columns] * factor + weights.reshape(
                    small // 8, 8, small
                ).sum(axis=0)
                sum_out[:, columns] = sum_out[:, columns] * factor + lax.dot_general(
                    value_refs[piece][pl.ds(start, small), :],
                    weights.astype(jnp.bfloat16),
                    (((0,), (0,)), ((), ())),
                    preferred_element_type=jnp.float32,
                )
                max_out[:, columns] = jnp.broadcast_to(new_max, (8, small))
                return carry

            lax.fori_loop(0, (piece_rows // small) * (rows // small), one_tile, 0)


def attend(norm, queries, keys, values, state, name, block=768, key_tile=512, query_tile=384):
    rows = queries.shape[0]
    pieces = len(keys)
    piece_rows = keys[0].shape[0]
    first = state is None
    scalar = pl.BlockSpec(memory_space=pltpu.SMEM)
    whole = pl.BlockSpec((piece_rows, DH), lambda i: (0, 0))
    state_specs = [
        scalar,
        pl.BlockSpec((DH, block), lambda i: (0, i)),
        pl.BlockSpec((8, block), lambda i: (0, i)),
        pl.BlockSpec((8, block), lambda i: (0, i)),
    ]
    in_specs = [scalar, pl.BlockSpec((block, 2 * DH), lambda i: (i, 0))] + [whole] * (2 * pieces)
    operands = [norm, queries, *keys, *values]
    aliases = {}
    if not first:
        aliases = {len(operands) + i: i for i in range(1, 4)}
        in_specs += state_specs
        operands += list(state)
    return pl.pallas_call(
        functools.partial(
            attend_kernel, pieces=pieces, first=first, key_tile=key_tile, query_tile=query_tile
        ),
        grid=(rows // block,),
        in_specs=in_specs,
        out_specs=state_specs,
        out_shape=[
            jax.ShapeDtypeStruct((1, 1), jnp.int32),
            jax.ShapeDtypeStruct((DH, rows), jnp.float32),
            jax.ShapeDtypeStruct((8, rows), jnp.float32),
            jax.ShapeDtypeStruct((8, rows), jnp.float32),
        ],
        scratch_shapes=[
            pltpu.VMEM((DH, pieces * piece_rows), jnp.bfloat16),
            pltpu.VMEM((2, pieces * piece_rows, query_tile), jnp.bfloat16),
            pltpu.SMEM((1,), jnp.int32),
        ],
        input_output_aliases=aliases,
        compiler_params=pltpu.CompilerParams(vmem_limit_bytes=48 * 2**20),
        name=name,
    )(*operands)


def finish_kernel(sum_a, total_a, max_a, sum_b, total_b, max_b, out_ref):
    joint = jnp.maximum(max_a[...], max_b[...])
    factor_a = jnp.exp2(max_a[...] - joint)
    factor_b = jnp.exp2(max_b[...] - joint)
    total = jnp.sum(total_a[...] * factor_a + total_b[...] * factor_b, axis=0, keepdims=True)
    summed = sum_a[...] * factor_a[:1] + sum_b[...] * factor_b[:1]
    out_ref[...] = (summed / total).T.astype(jnp.bfloat16)


def finish(own, received):
    rows = own[0].shape[1]
    return pl.pallas_call(
        finish_kernel,
        in_specs=[pl.BlockSpec(memory_space=pltpu.VMEM)] * 6,
        out_specs=pl.BlockSpec(memory_space=pltpu.VMEM),
        out_shape=jax.ShapeDtypeStruct((rows, DH), jnp.bfloat16),
        compiler_params=pltpu.CompilerParams(vmem_limit_bytes=48 * 2**20),
        name="finish",
    )(*own, *received)


def to_heads(x):
    return lax.all_to_all(x, PLANE, split_axis=1, concat_axis=0, tiled=True)


def body(queries, keys, values, masked_at, mask_query, mask_key, mask_value):
    local_rows = queries.shape[0]
    first_row = lax.axis_index(("pb", "kv", "ha")) * local_rows
    positions = first_row + jnp.arange(local_rows, dtype=jnp.int32)
    masked_flags = jnp.any(positions[:, None] == masked_at[None, :], axis=1)
    key_used = jnp.where(masked_flags[:, None], rotated(mask_key, positions), keys)
    value_used = jnp.where(masked_flags[:, None], mask_value[None, :], values)
    query_used = jnp.where(masked_flags[:, None], rotated(mask_query, positions), queries)

    k_own = to_heads(key_used)
    v_own = to_heads(value_used)
    k_left = along_x(k_own, 1)
    k_right = along_x(k_own, -1)
    v_left = along_x(v_own, 1)
    v_right = along_x(v_own, -1)
    k_far = along_x(k_left, 1)
    v_far = along_x(v_right, -1)

    q_own = to_heads(query_used)
    q_other = other_core(q_own)
    own, own_norm = split_queries(q_own)
    other, other_norm = split_queries(q_other)

    own_state = attend(own_norm, own, [k_own], [v_own], None, "own_0")
    other_state = attend(other_norm, other, [k_own], [v_own], None, "other_0")
    near_k, near_v = [k_left, k_right], [v_left, v_right]
    own_state = attend(own_norm, own, near_k, near_v, own_state, "own_1")
    other_state = attend(other_norm, other, near_k, near_v, other_state, "other_1")
    other_state = attend(other_norm, other, [k_far], [v_far], other_state, "other_2")
    received = [other_core(x) for x in other_state[1:]]
    own_state = attend(own_norm, own, [k_far], [v_far], own_state, "own_2")
    rows = finish(own_state[1:], received)
    return lax.all_to_all(rows, PLANE, split_axis=0, concat_axis=1, tiled=True)


def solution(mesh):
    split = P(("pb", "kv", "ha"), None)
    return jax.shard_map(
        body,
        mesh=mesh,
        in_specs=(split, split, split, P(), P(), P(), P()),
        out_specs=split,
        check_vma=False,
    )
```

```python
import functools
import math

import jax
import jax.numpy as jnp
from jax import lax
from jax.experimental import pallas as pl
from jax.experimental.pallas import tpu as pltpu
from jax.sharding import PartitionSpec as P

DH = 128
HEADS = 16
ROPE_THETA = 500000.0
VERY_NEGATIVE = -1e30
LEAST_TOTAL = 2.0**-60
LARGEST_TOTAL = 2.0**110
SCORE_SCALE = math.log2(math.e) / math.sqrt(DH)
CONTRACT_LAST = (((1,), (1,)), ((), ()))
PLANE = ("kv", "ha")
VMEM = pl.BlockSpec(memory_space=pltpu.VMEM)
SUMS = pl.ds(0, DH)
TOTALS = pl.ds(DH, 8)
MAXIMA = pl.ds(DH + 8, 8)
STATE_ROWS = DH + 16


def along_x(x, step):
    return lax.ppermute(x, "pb", [(i, (i + 2 * step) % 8) for i in range(8)])


def other_core(x):
    return lax.ppermute(x, "pb", [(i, i ^ 1) for i in range(8)])


def params():
    return pltpu.CompilerParams(vmem_limit_bytes=48 * 2**20)


def rotary_tables(positions):
    halves = DH // 2
    exponent = jnp.arange(halves, dtype=jnp.float32) * (2.0 / DH)
    inverse = 1.0 / ROPE_THETA**exponent
    angles = positions.astype(jnp.float32)[:, None] * inverse[None, :]
    return jnp.cos(angles), jnp.sin(angles)


def place_kernel(first_ref, masked_at_ref, cos_ref, sin_ref, mask_ref, q_ref, k_ref, v_ref, out_ref):
    rows = q_ref.shape[0]
    positions = first_ref[0] + lax.broadcasted_iota(jnp.int32, (rows, DH), 0)
    hits = jnp.zeros((rows, DH), jnp.float32)
    for line in range(masked_at_ref.shape[0]):
        hits = jnp.where(positions == masked_at_ref[line : line + 1, :], 1.0, hits)
    masked = jnp.broadcast_to(jnp.max(hits, axis=1, keepdims=True), (rows, DH)) > 0.0
    cosine = jnp.concatenate([cos_ref[...], cos_ref[...]], axis=1)
    sine = jnp.concatenate([-sin_ref[...], sin_ref[...]], axis=1)
    plain = [mask_ref[part].astype(jnp.float32) for part in range(3)]
    swapped = [pltpu.roll(part, DH // 2, 1) for part in plain[:2]]
    for head in range(HEADS):
        columns = pl.ds(head * DH, DH)
        for part, ref in enumerate((q_ref, k_ref, v_ref)):
            fill = plain[part][head : head + 1, :]
            if part < 2:
                fill = fill * cosine + swapped[part][head : head + 1, :] * sine
            chosen = jnp.where(masked, fill, ref[:, columns].astype(jnp.float32))
            out_ref[head, pl.ds(part * rows, rows), :] = chosen.astype(jnp.bfloat16)


def place(first_row, masked_at, tables, masks, queries, keys, values):
    rows = queries.shape[0]
    return pl.pallas_call(
        place_kernel,
        in_specs=[pl.BlockSpec(memory_space=pltpu.SMEM)] + [VMEM] * 7,
        out_specs=VMEM,
        out_shape=jax.ShapeDtypeStruct((HEADS, 3 * rows, DH), jnp.bfloat16),
        compiler_params=params(),
        name="place",
    )(first_row.reshape(1), masked_at.reshape(-1, DH), *tables, masks, queries, keys, values)


def split_queries(raw_ref, out_ref):
    scaled = raw_ref[...].reshape(-1, DH).astype(jnp.float32) * SCORE_SCALE
    high = scaled.astype(jnp.bfloat16)
    out_ref[:, :DH] = high
    out_ref[:, DH:] = (scaled - high.astype(jnp.float32)).astype(jnp.bfloat16)


def key_tile(piece_ref, start, blocks):
    rows = piece_ref.shape[1] // 2
    return piece_ref[pl.ds(start, blocks), pl.ds(0, rows), :].reshape(blocks * rows, DH)


def value_tile(piece_ref, start, blocks):
    rows = piece_ref.shape[1] // 2
    return piece_ref[pl.ds(start, blocks), pl.ds(rows, rows), :].reshape(blocks * rows, DH)


def scores_of(keys, queries):
    doubled = jnp.concatenate([keys, keys], axis=1)
    return lax.dot_general(doubled, queries, CONTRACT_LAST, preferred_element_type=jnp.float32)


def turn_values(pieces, turned_ref):
    at = 0
    for piece in pieces:
        values = value_tile(piece, 0, piece.shape[0])
        turned_ref[:, pl.ds(at, values.shape[0])] = values.T
        at += values.shape[0]


def attend_block(queries, columns, pieces, state_in, state_out, turned_ref, weight_ref, tile_blocks):
    width = weight_ref.shape[1]
    total = None if state_in is None else state_in[TOTALS, columns]
    at = 0
    for piece in pieces:
        for start in range(0, piece.shape[0], tile_blocks):
            scores = scores_of(key_tile(piece, start, tile_blocks), queries)
            weights = jnp.exp2(scores)
            rows = weights.shape[0]
            part = weights.reshape(rows // 8, 8, width).sum(axis=0)
            total = part if total is None else total + part
            weight_ref[pl.ds(at, rows), :] = weights.astype(jnp.bfloat16)
            at += rows
    summed = jnp.dot(turned_ref[...], weight_ref[...], preferred_element_type=jnp.float32)
    if state_in is not None:
        summed = summed + state_in[SUMS, columns]
    state_out[SUMS, columns] = summed
    state_out[TOTALS, columns] = total


def attend_kernel(*refs, sets, pieces, first, width, unroll, tile_blocks):
    queries = refs[:sets]
    keys = refs[sets : sets + pieces]
    rest = refs[sets + pieces :]
    states_in = [None] * sets
    if first:
        raw, queries, rest = queries, rest[:sets], rest[sets:]
        for raw_ref, query_ref in zip(raw, queries):
            split_queries(raw_ref, query_ref)
    else:
        states_in, rest = rest[:sets], rest[sets:]
    states_out = rest[:sets]
    turned_ref, *weight_refs = rest[sets:]
    turn_values(keys, turned_ref)
    for query_ref, state_in, state_out in zip(queries, states_in, states_out):

        def step(index, carry):
            for part in range(unroll):
                columns = pl.ds(pl.multiple_of((index * unroll + part) * width, width), width)
                attend_block(
                    query_ref[columns, :], columns, keys, state_in, state_out, turned_ref,
                    weight_refs[part % 2], tile_blocks,
                )
            return carry

        lax.fori_loop(0, query_ref.shape[0] // (width * unroll), step, 0)


def scratch_for(pieces, width):
    count = sum(piece.shape[0] * piece.shape[1] // 2 for piece in pieces)
    return [pltpu.VMEM((DH, count), jnp.bfloat16)] + [pltpu.VMEM((count, width), jnp.bfloat16)] * 2


def attend(queries, pieces, states, name, width=512, unroll=1, tile_blocks=4):
    first = states is None
    operands = [*queries, *pieces, *(states or ())]
    rows = queries[0].size // (DH if first else 2 * DH)
    outs = [jax.ShapeDtypeStruct((STATE_ROWS, rows), jnp.float32)] * len(queries)
    if first:
        outs = [jax.ShapeDtypeStruct((rows, 2 * DH), jnp.bfloat16)] * len(queries) + outs
    return pl.pallas_call(
        functools.partial(
            attend_kernel, sets=len(queries), pieces=len(pieces), first=first, width=width, unroll=unroll,
            tile_blocks=tile_blocks,
        ),
        in_specs=[VMEM] * len(operands),
        out_specs=[VMEM] * len(outs),
        out_shape=outs,
        scratch_shapes=scratch_for(pieces, width),
        compiler_params=params(),
        name=name,
    )(*operands)


def attend_last_kernel(*refs, pieces, others, width, unroll, tile_blocks):
    query_ref = refs[0]
    keys = refs[1 : 1 + pieces]
    other_keys = refs[1 + pieces : 1 + pieces + others]
    state_in, state_out, turned_ref, *weight_refs = refs[1 + pieces + others :]
    rows = query_ref.shape[0]
    turn_values(keys, turned_ref)

    def step(index, carry):
        for part in range(unroll):
            columns = pl.ds(pl.multiple_of((index * unroll + part) * width, width), width)
            attend_block(
                query_ref[columns, :], columns, keys, state_in, state_out, turned_ref, weight_refs[part % 2],
                tile_blocks,
            )
        return carry

    lax.fori_loop(0, rows // (width * unroll), step, 0)
    state_out[MAXIMA, :] = jnp.zeros((8, rows), jnp.float32)
    totals = jnp.sum(state_out[TOTALS, :], axis=0, keepdims=True)
    inside = (totals >= LEAST_TOTAL) & (totals <= LARGEST_TOTAL)
    outside = jnp.max(jnp.where(inside, 0.0, 1.0))

    @pl.when(outside > 0.0)
    def _():
        small = 128
        state_out[pl.ds(0, DH + 8), :] = jnp.zeros((DH + 8, rows), jnp.float32)
        state_out[MAXIMA, :] = jnp.full((8, rows), VERY_NEGATIVE, jnp.float32)
        for piece in [*other_keys, *keys]:

            def one_tile(index, carry):
                block = index // (rows // small)
                columns = pl.ds(pl.multiple_of((index % (rows // small)) * small, small), small)
                scores = scores_of(key_tile(piece, block, 1), query_ref[columns, :])
                old_max = state_out[pl.ds(DH + 8, 1), columns]
                new_max = jnp.maximum(old_max, jnp.max(scores, axis=0, keepdims=True))
                factor = jnp.exp2(old_max - new_max)
                weights = jnp.exp2(scores - new_max)
                part = weights.reshape(weights.shape[0] // 8, 8, small).sum(axis=0)
                state_out[TOTALS, columns] = state_out[TOTALS, columns] * factor + part
                state_out[SUMS, columns] = state_out[SUMS, columns] * factor + lax.dot_general(
                    value_tile(piece, block, 1),
                    weights.astype(jnp.bfloat16),
                    (((0,), (0,)), ((), ())),
                    preferred_element_type=jnp.float32,
                )
                state_out[MAXIMA, columns] = jnp.broadcast_to(new_max, (8, small))
                return carry

            lax.fori_loop(0, piece.shape[0] * (rows // small), one_tile, 0)


def attend_last(queries, pieces, others, state, name, width=512, unroll=1, tile_blocks=4):
    operands = [queries, *pieces, *others, state]
    return pl.pallas_call(
        functools.partial(
            attend_last_kernel, pieces=len(pieces), others=len(others), width=width, unroll=unroll,
            tile_blocks=tile_blocks,
        ),
        in_specs=[VMEM] * len(operands),
        out_specs=VMEM,
        out_shape=jax.ShapeDtypeStruct((STATE_ROWS, queries.shape[0]), jnp.float32),
        scratch_shapes=scratch_for(pieces, width),
        compiler_params=params(),
        name=name,
    )(*operands)


def finish_kernel(own_ref, received_ref, out_ref):
    own_max, received_max = own_ref[MAXIMA, :], received_ref[MAXIMA, :]
    joint = jnp.maximum(own_max, received_max)
    own_factor = jnp.exp2(own_max - joint)
    received_factor = jnp.exp2(received_max - joint)
    total = own_ref[TOTALS, :] * own_factor + received_ref[TOTALS, :] * received_factor
    inverse = 1.0 / jnp.sum(total, axis=0, keepdims=True)
    summed = own_ref[SUMS, :] * (own_factor[:1] * inverse) + received_ref[SUMS, :] * (received_factor[:1] * inverse)
    out_ref[...] = summed.T.astype(jnp.bfloat16)


def finish(own, received):
    return pl.pallas_call(
        finish_kernel,
        in_specs=[VMEM] * 2,
        out_specs=VMEM,
        out_shape=jax.ShapeDtypeStruct((own.shape[1], DH), jnp.bfloat16),
        compiler_params=params(),
        name="finish",
    )(own, received)


def swap_plane(x):
    return lax.all_to_all(x, PLANE, split_axis=0, concat_axis=0, tiled=True)


def after_all(xs, *earlier):
    tied = lax.optimization_barrier((*xs, *earlier))
    return [list(tied[: len(xs)]), *tied[len(xs) :]]


def after(x, *earlier):
    return lax.optimization_barrier((x, *earlier))[0]


def body(queries, keys, values, masked_at, mask_query, mask_key, mask_value):
    local_rows = queries.shape[0]
    first_row = lax.axis_index(("pb", "kv", "ha")) * local_rows
    positions = first_row + jnp.arange(local_rows, dtype=jnp.int32)
    masks = jnp.stack([mask.reshape(HEADS, DH) for mask in (mask_query, mask_key, mask_value)])
    placed = place(first_row, masked_at, rotary_tables(positions), masks, queries, keys, values)
    gathered = swap_plane(placed)
    q_own = gathered[:, :local_rows]
    half = HEADS // 2
    kv_a = gathered[:half, local_rows:]
    kv_b = gathered[half:, local_rows:]

    q_other = other_core(q_own)
    left_a = along_x(kv_a, 1)
    right_b = along_x(kv_b, -1)
    left_b = along_x(kv_b, 1)
    right_a = along_x(kv_a, -1)
    own, other, *states = attend([q_own, q_other], [kv_a, kv_b], None, "attend_own")
    both = [own, other]

    near, *states = after_all([left_a, right_b], *states)
    quarter = half // 2
    far_first = [along_x(near[0][:quarter], 1), along_x(near[1][:quarter], -1)]
    far_second = [along_x(near[0][quarter:], 1), along_x(near[1][quarter:], -1)]
    states = attend(both, near, states, "attend_near")

    near_second, *states = after_all([left_b, right_a], *states)
    states = attend(both, near_second, states, "attend_near_second")

    far_first, *states = after_all(far_first, *states)
    states = attend(both, far_first, states, "attend_far")

    far_second, *states = after_all(far_second, *states)
    earlier = [kv_a, kv_b, *near, *near_second, *far_first]
    other_state = attend_last(other, far_second, earlier, states[1], "attend_last_other")
    received = other_core(other_state)
    own_state = attend_last(own, far_second, earlier, after(states[0], other_state), "attend_last_own")
    rows = finish(own_state, received)
    out = swap_plane(rows.reshape(HEADS, local_rows, DH))
    return out.transpose(1, 0, 2).reshape(local_rows, HEADS * DH)


def solution(mesh):
    split = P(("pb", "kv", "ha"), None)
    return jax.shard_map(
        body,
        mesh=mesh,
        in_specs=(split, split, split, P(), P(), P(), P()),
        out_specs=split,
        check_vma=False,
    )
```

```python
import functools
import math

import jax
import jax.numpy as jnp
from jax import lax
from jax.experimental import pallas as pl
from jax.experimental.pallas import tpu as pltpu
from jax.sharding import PartitionSpec as P


DH = 128
HEADS = 16
ROPE_THETA = 500000.0
VERY_NEGATIVE = -1e30
LEAST_TOTAL = 2.0**-60
LARGEST_TOTAL = 2.0**110
SCORE_SCALE = math.log2(math.e) / math.sqrt(DH)
CONTRACT_LAST = (((1,), (1,)), ((), ()))
PLANE = ("kv", "ha")
VMEM = pl.BlockSpec(memory_space=pltpu.VMEM)
SUMS = pl.ds(0, DH)
TOTALS = pl.ds(DH, 8)
MAXIMA = pl.ds(DH + 8, 8)
STATE_ROWS = DH + 16


def along_x(x, step):
    return lax.ppermute(x, "pb", [(i, (i + 2 * step) % 8) for i in range(8)])


def other_core(x):
    return lax.ppermute(x, "pb", [(i, i ^ 1) for i in range(8)])


def params():
    return pltpu.CompilerParams(vmem_limit_bytes=48 * 2**20)


def rotary_tables(positions):
    halves = DH // 2
    exponent = jnp.arange(halves, dtype=jnp.float32) * (2.0 / DH)
    inverse = 1.0 / ROPE_THETA**exponent
    angles = positions.astype(jnp.float32)[:, None] * inverse[None, :]
    return jnp.cos(angles), jnp.sin(angles)


def place_kernel(
    first_ref, cos_ref, sin_ref, at_hbm, mq_hbm, mk_hbm, mv_hbm, q_hbm, k_hbm, v_hbm, out_ref,
    at_ref, mq_ref, mk_ref, mv_ref, q_ref, k_ref, v_ref, arrived,
):
    sources = (at_hbm, mq_hbm, mk_hbm, mv_hbm, q_hbm, k_hbm, v_hbm)
    landings = (at_ref, mq_ref, mk_ref, mv_ref, q_ref, k_ref, v_ref)
    copies = [pltpu.make_async_copy(s, d, arrived.at[i]) for i, (s, d) in enumerate(zip(sources, landings))]
    for copy in copies:
        copy.start()
    rows = q_ref.shape[0]
    positions = first_ref[0] + lax.broadcasted_iota(jnp.int32, (rows, DH), 0)
    cosine = jnp.concatenate([cos_ref[...], cos_ref[...]], axis=1)
    sine = jnp.concatenate([-sin_ref[...], sin_ref[...]], axis=1)
    for copy in copies[:4]:
        copy.wait()
    hits = jnp.zeros((rows, DH), jnp.float32)
    for line in range(at_ref.shape[0]):
        hits = jnp.where(positions == at_ref[line : line + 1, :], 1.0, hits)
    masked = jnp.broadcast_to(jnp.max(hits, axis=1, keepdims=True), (rows, DH)) > 0.0
    for part, (mask_ref, ref) in enumerate(((mq_ref, q_ref), (mk_ref, k_ref), (mv_ref, v_ref))):
        plain = mask_ref[...].astype(jnp.float32)
        swapped = pltpu.roll(plain, DH // 2, 1)
        copies[4 + part].wait()
        for head in range(HEADS):
            fill = plain[head : head + 1, :]
            if part < 2:
                fill = fill * cosine + swapped[head : head + 1, :] * sine
            chosen = jnp.where(masked, fill, ref[:, pl.ds(head * DH, DH)].astype(jnp.float32))
            out_ref[head, pl.ds(part * rows, rows), :] = chosen.astype(jnp.bfloat16)


def place(first_row, masked_at, tables, masks, queries, keys, values):
    rows = queries.shape[0]
    fetched = [masked_at.reshape(-1, DH), *(mask.reshape(HEADS, DH) for mask in masks), queries, keys, values]
    return pl.pallas_call(
        place_kernel,
        in_specs=[pl.BlockSpec(memory_space=pltpu.SMEM)] + [VMEM] * 2
        + [pl.BlockSpec(memory_space=pltpu.HBM)] * len(fetched),
        out_specs=VMEM,
        out_shape=jax.ShapeDtypeStruct((HEADS, 3 * rows, DH), jnp.bfloat16),
        scratch_shapes=[pltpu.VMEM(x.shape, x.dtype) for x in fetched]
        + [pltpu.SemaphoreType.DMA((len(fetched),))],
        compiler_params=params(),
        name="place",
    )(first_row.reshape(1), *tables, *(pltpu.with_memory_space_constraint(x, pltpu.HBM) for x in fetched))


def split_queries(raw_ref, out_ref):
    scaled = raw_ref[...].reshape(-1, DH).astype(jnp.float32) * SCORE_SCALE
    high = scaled.astype(jnp.bfloat16)
    out_ref[:, :DH] = high
    out_ref[:, DH:] = (scaled - high.astype(jnp.float32)).astype(jnp.bfloat16)


def key_tile(piece_ref, start, blocks):
    rows = piece_ref.shape[1] // 2
    return piece_ref[pl.ds(start, blocks), pl.ds(0, rows), :].reshape(blocks * rows, DH)


def value_tile(piece_ref, start, blocks):
    rows = piece_ref.shape[1] // 2
    return piece_ref[pl.ds(start, blocks), pl.ds(rows, rows), :].reshape(blocks * rows, DH)


def scores_of(keys, queries):
    doubled = jnp.concatenate([keys, keys], axis=1)
    return lax.dot_general(doubled, queries, CONTRACT_LAST, preferred_element_type=jnp.float32)


def turn_values(pieces, turned_ref):
    at = 0
    for piece in pieces:
        values = value_tile(piece, 0, piece.shape[0])
        turned_ref[:, pl.ds(at, values.shape[0])] = values.T
        at += values.shape[0]


def attend_block(queries, columns, pieces, state_in, state_out, turned_ref, weight_ref, tile_blocks):
    width = weight_ref.shape[1]
    total = None if state_in is None else state_in[TOTALS, columns]
    at = 0
    for piece in pieces:
        for start in range(0, piece.shape[0], tile_blocks):
            scores = scores_of(key_tile(piece, start, tile_blocks), queries)
            weights = jnp.exp2(scores)
            rows = weights.shape[0]
            part = weights.reshape(rows // 8, 8, width).sum(axis=0)
            total = part if total is None else total + part
            weight_ref[pl.ds(at, rows), :] = weights.astype(jnp.bfloat16)
            at += rows
    summed = jnp.dot(turned_ref[...], weight_ref[...], preferred_element_type=jnp.float32)
    if state_in is not None:
        summed = summed + state_in[SUMS, columns]
    state_out[SUMS, columns] = summed
    state_out[TOTALS, columns] = total


def attend_kernel(*refs, sets, pieces, first, width, tile_blocks):
    queries = refs[:sets]
    keys = refs[sets : sets + pieces]
    rest = refs[sets + pieces :]
    states_in = [None] * sets
    if first:
        raw, queries, rest = queries, rest[:sets], rest[sets:]
        for raw_ref, query_ref in zip(raw, queries):
            split_queries(raw_ref, query_ref)
    else:
        states_in, rest = rest[:sets], rest[sets:]
    states_out = rest[:sets]
    turned_ref, weight_ref = rest[sets:]
    turn_values(keys, turned_ref)
    for query_ref, state_in, state_out in zip(queries, states_in, states_out):

        for start in range(0, query_ref.shape[0], width):
            columns = pl.ds(start, width)
            attend_block(
                query_ref[columns, :], columns, keys, state_in, state_out, turned_ref, weight_ref, tile_blocks
            )


def scratch_for(pieces, width):
    count = sum(piece.shape[0] * piece.shape[1] // 2 for piece in pieces)
    return [pltpu.VMEM((DH, count), jnp.bfloat16), pltpu.VMEM((count, width), jnp.bfloat16)]


def attend(queries, pieces, states, width=1536, tile_blocks=4):
    first = states is None
    operands = [*queries, *pieces, *(states or ())]
    rows = queries[0].size // (DH if first else 2 * DH)
    outs = [jax.ShapeDtypeStruct((STATE_ROWS, rows), jnp.float32)] * len(queries)
    if first:
        outs = [jax.ShapeDtypeStruct((rows, 2 * DH), jnp.bfloat16)] * len(queries) + outs
    return pl.pallas_call(
        functools.partial(
            attend_kernel, sets=len(queries), pieces=len(pieces), first=first, width=width,
            tile_blocks=tile_blocks,
        ),
        in_specs=[VMEM] * len(operands),
        out_specs=[VMEM] * len(outs),
        out_shape=outs,
        scratch_shapes=scratch_for(pieces, width),
        compiler_params=params(),
    )(*operands)


def attend_last_kernel(*refs, pieces, others, width, tile_blocks):
    query_ref = refs[0]
    keys = refs[1 : 1 + pieces]
    other_keys = refs[1 + pieces : 1 + pieces + others]
    state_in, state_out, turned_ref, weight_ref = refs[1 + pieces + others :]
    rows = query_ref.shape[0]
    turn_values(keys, turned_ref)

    for start in range(0, rows, width):
        columns = pl.ds(start, width)
        attend_block(
            query_ref[columns, :], columns, keys, state_in, state_out, turned_ref, weight_ref, tile_blocks
        )
    state_out[MAXIMA, :] = jnp.zeros((8, rows), jnp.float32)
    totals = jnp.sum(state_out[TOTALS, :], axis=0, keepdims=True)
    inside = (totals >= LEAST_TOTAL) & (totals <= LARGEST_TOTAL)
    outside = jnp.max(jnp.where(inside, 0.0, 1.0))

    @pl.when(outside > 0.0)
    def _():
        small = 128
        state_out[pl.ds(0, DH + 8), :] = jnp.zeros((DH + 8, rows), jnp.float32)
        state_out[MAXIMA, :] = jnp.full((8, rows), VERY_NEGATIVE, jnp.float32)
        for piece in [*other_keys, *keys]:

            def one_tile(index, carry):
                block = index // (rows // small)
                columns = pl.ds(pl.multiple_of((index % (rows // small)) * small, small), small)
                scores = scores_of(key_tile(piece, block, 1), query_ref[columns, :])
                old_max = state_out[pl.ds(DH + 8, 1), columns]
                new_max = jnp.maximum(old_max, jnp.max(scores, axis=0, keepdims=True))
                factor = jnp.exp2(old_max - new_max)
                weights = jnp.exp2(scores - new_max)
                part = weights.reshape(weights.shape[0] // 8, 8, small).sum(axis=0)
                state_out[TOTALS, columns] = state_out[TOTALS, columns] * factor + part
                state_out[SUMS, columns] = state_out[SUMS, columns] * factor + lax.dot_general(
                    value_tile(piece, block, 1),
                    weights.astype(jnp.bfloat16),
                    (((0,), (0,)), ((), ())),
                    preferred_element_type=jnp.float32,
                )
                state_out[MAXIMA, columns] = jnp.broadcast_to(new_max, (8, small))
                return carry

            lax.fori_loop(0, piece.shape[0] * (rows // small), one_tile, 0)


def attend_last(queries, pieces, others, state, width=1536, tile_blocks=4):
    operands = [queries, *pieces, *others, state]
    return pl.pallas_call(
        functools.partial(
            attend_last_kernel, pieces=len(pieces), others=len(others), width=width,
            tile_blocks=tile_blocks,
        ),
        in_specs=[VMEM] * len(operands),
        out_specs=VMEM,
        out_shape=jax.ShapeDtypeStruct((STATE_ROWS, queries.shape[0]), jnp.float32),
        scratch_shapes=scratch_for(pieces, width),
        compiler_params=params(),
    )(*operands)


def finish_kernel(own_ref, received_ref, out_ref):
    own_max, received_max = own_ref[MAXIMA, :], received_ref[MAXIMA, :]
    joint = jnp.maximum(own_max, received_max)
    own_factor = jnp.exp2(own_max - joint)
    received_factor = jnp.exp2(received_max - joint)
    total = own_ref[TOTALS, :] * own_factor + received_ref[TOTALS, :] * received_factor
    inverse = 1.0 / jnp.sum(total, axis=0, keepdims=True)
    summed = own_ref[SUMS, :] * (own_factor[:1] * inverse) + received_ref[SUMS, :] * (received_factor[:1] * inverse)
    out_ref[...] = summed.T.astype(jnp.bfloat16)


def finish(own, received):
    return pl.pallas_call(
        finish_kernel,
        in_specs=[VMEM] * 2,
        out_specs=VMEM,
        out_shape=jax.ShapeDtypeStruct((own.shape[1], DH), jnp.bfloat16),
        compiler_params=params(),
        name="finish",
    )(own, received)


def swap_plane(x):
    return lax.all_to_all(x, PLANE, split_axis=0, concat_axis=0, tiled=True)


def after_all(xs, *earlier):
    tied = lax.optimization_barrier((*xs, *earlier))
    return [list(tied[: len(xs)]), *tied[len(xs) :]]


def after(x, *earlier):
    return lax.optimization_barrier((x, *earlier))[0]


def attention(queries, keys, values, masked_at, mask_query, mask_key, mask_value):
    local_rows = queries.shape[0]
    first_row = lax.axis_index(("pb", "kv", "ha")) * local_rows
    positions = first_row + jnp.arange(local_rows, dtype=jnp.int32)
    masks = (mask_query, mask_key, mask_value)
    placed = place(first_row, masked_at, rotary_tables(positions), masks, queries, keys, values)
    gathered = swap_plane(placed)
    half = HEADS // 2
    q_own = gathered[:, :local_rows]
    kv_a, kv_b = gathered[:half, local_rows:], gathered[half:, local_rows:]
    left_a = along_x(kv_a, 1)
    right_b = along_x(kv_b, -1)
    q_other = other_core(q_own)
    own, own_state = attend([q_own], [kv_a, kv_b], None)
    (late_b, late_a), own_state = after_all([kv_b, kv_a], own_state)
    left_b = along_x(late_b, 1)
    right_a = along_x(late_a, -1)
    other, other_state = attend([q_other], [kv_a, kv_b], None)

    near, own_state, other_state = after_all([left_a, right_b], own_state, other_state)
    far_a = along_x(near[0], 1)
    far_b = along_x(near[1], -1)
    (own_state,) = attend([own], near, [own_state])
    (other_state,) = attend([other], near, [other_state])

    second, own_state, other_state = after_all([left_b, right_a], own_state, other_state)
    (own_state,) = attend([own], second, [own_state])
    (other_state,) = attend([other], second, [other_state])

    far, own_state, other_state = after_all([far_a, far_b], own_state, other_state)
    earlier = [kv_a, kv_b, *near, *second]
    other_state = attend_last(other, far, earlier, other_state)
    received = other_core(other_state)
    own_state = attend_last(own, far, earlier, after(own_state, other_state))
    rows = finish(own_state, received)
    out = swap_plane(rows.reshape(HEADS, local_rows, DH))
    return out.transpose(1, 0, 2).reshape(local_rows, HEADS * DH)


def solution(mesh):
    split = P(("pb", "kv", "ha"), None)
    return jax.shard_map(
        attention,
        mesh=mesh,
        in_specs=(split, split, split, P(), P(), P(), P()),
        out_specs=split,
        check_vma=False,
    )
```
